8 devices in a mesh: data: 1 (over z), fsdp: 2 (over y), ep: 4 (over x, core).
Axes of the slice: x: 2, y: 2, z: 1, core: 2. Of those that a mesh axis runs over, the one named last changes fastest.
Arguments:
- x_in: bfloat16 [64, 512, 2048], P(('data', 'fsdp', 'ep'))
- w_qkv: bfloat16 [2048, 6144], P('fsdp')
- w_out: bfloat16 [2048, 2048], P('fsdp')
- w_gate: bfloat16 [60, 2048, 1408], P('ep', 'fsdp')
- w_up: bfloat16 [60, 2048, 1408], P('ep', 'fsdp')
- w_down: bfloat16 [60, 1408, 2048], P('ep', None, 'fsdp')
- ws_gate: bfloat16 [2048, 5632], P('fsdp')
- ws_up: bfloat16 [2048, 5632], P('fsdp')
- ws_down: bfloat16 [5632, 2048], P(None, 'fsdp')
- expert_ids: int32 [64, 512, 4], P(('data', 'fsdp', 'ep'))
- slot_ids: int32 [64, 512, 4], P(('data', 'fsdp', 'ep'))
- gate_vals: bfloat16 [64, 512, 4], P(('data', 'fsdp', 'ep'))
Outputs:
- output: bfloat16 [64, 512, 2048], P(('data', 'fsdp', 'ep'))
All inputs are finite; a program needn't handle non-finite values.
Results may differ from the reference program's by a relative error of at most 0.00870369.
Values are sent between devices in bfloat16 or wider.
A program may use at most 1 GiB of HBM per device.

```python
import jax
import jax.numpy as jnp
from jax import lax

MODEL_DIM = 2048
NUM_HEADS = 16
HEAD_DIM = 128
NUM_EXPERTS = 60
TOP_K = 4
EXPERT_FF = 1408
SHARED_FF = 5632
BATCH_DEV = 8
SEQ_LEN = 512
GROUP_DEVS = 8
TOKENS = BATCH_DEV * SEQ_LEN
CAPACITY = ((5 * TOKENS * TOP_K) // (4 * NUM_EXPERTS) + 7) // 8 * 8
ROPE_BASE = 10000.0
EPSILON = 1e-6


def normal_weight(rand_key, weight_shape, fan_in):
    scaled = jax.random.normal(rand_key, weight_shape, jnp.float32) * (fan_in ** -0.5)
    return scaled.astype(jnp.bfloat16)


def draw_routing(rand_key):
    score_key, bias_key, hot_key = jax.random.split(rand_key, 3)
    expert_iota = jnp.arange(NUM_EXPERTS, dtype=jnp.int32)
    scores = jax.random.randint(score_key, (GROUP_DEVS, TOKENS, NUM_EXPERTS), 0, 1000, dtype=jnp.int32)
    expert_bias = jax.random.randint(bias_key, (GROUP_DEVS, 1, NUM_EXPERTS), 0, 500, dtype=jnp.int32)
    hot_expert = jax.random.randint(hot_key, (GROUP_DEVS, 1, 1), 0, NUM_EXPERTS, dtype=jnp.int32)
    total_score = scores + expert_bias + jnp.where(expert_iota == hot_expert, 2000, 0)
    ranked = total_score * NUM_EXPERTS + expert_iota
    chosen = lax.top_k(ranked, TOP_K)[1].astype(jnp.int32)
    flat_ids = chosen.reshape(GROUP_DEVS, TOKENS * TOP_K)

    def device_slots(dev_ids):
        onehot = (dev_ids[:, None] == expert_iota[None, :]).astype(jnp.int32)
        running = jnp.cumsum(onehot, axis=0) - 1
        position = jnp.sum(running * onehot, axis=1)
        return jnp.where(position < CAPACITY, position, -1)

    slot_table = lax.map(device_slots, flat_ids)
    route_shape = (GROUP_DEVS * BATCH_DEV, SEQ_LEN, TOP_K)
    return chosen.reshape(route_shape), slot_table.reshape(route_shape)


def setup_inputs(seed: int = 0, part: int = 0) -> dict:
    weight_keys = jax.random.split(jax.random.key(seed), 8)
    part_keys = jax.random.split(jax.random.fold_in(jax.random.key(seed + 1), part), 3)
    n_seqs = GROUP_DEVS * BATCH_DEV
    expert_ids, slot_ids = draw_routing(part_keys[1])
    x_in = jax.random.normal(part_keys[0], (n_seqs, SEQ_LEN, MODEL_DIM), jnp.float32).astype(jnp.bfloat16)
    gate_vals = jax.random.uniform(part_keys[2], (n_seqs, SEQ_LEN, TOP_K), jnp.float32, 0.25, 1.0).astype(jnp.bfloat16)
    return {"x_in": x_in, "w_qkv": normal_weight(weight_keys[0], (MODEL_DIM, 3 * NUM_HEADS * HEAD_DIM), MODEL_DIM), "w_out": normal_weight(weight_keys[1], (NUM_HEADS * HEAD_DIM, MODEL_DIM), NUM_HEADS * HEAD_DIM), "w_gate": normal_weight(weight_keys[2], (NUM_EXPERTS, MODEL_DIM, EXPERT_FF), MODEL_DIM), "w_up": normal_weight(weight_keys[3], (NUM_EXPERTS, MODEL_DIM, EXPERT_FF), MODEL_DIM), "w_down": normal_weight(weight_keys[4], (NUM_EXPERTS, EXPERT_FF, MODEL_DIM), EXPERT_FF), "ws_gate": normal_weight(weight_keys[5], (MODEL_DIM, SHARED_FF), MODEL_DIM), "ws_up": normal_weight(weight_keys[6], (MODEL_DIM, SHARED_FF), MODEL_DIM), "ws_down": normal_weight(weight_keys[7], (SHARED_FF, MODEL_DIM), SHARED_FF), "expert_ids": expert_ids, "slot_ids": slot_ids, "gate_vals": gate_vals}


def rms_norm(values):
    vals_f32 = values.astype(jnp.float32)
    mean_sq = jnp.mean(vals_f32 * vals_f32, axis=-1, keepdims=True)
    return (vals_f32 * lax.rsqrt(mean_sq + EPSILON)).astype(jnp.bfloat16)


def rotary_embed(heads_in, positions):
    half_dim = HEAD_DIM // 2
    inv_freq = ROPE_BASE ** (-jnp.arange(half_dim).astype(jnp.float32) * (2.0 / HEAD_DIM))
    angles = positions[:, None] * inv_freq[None, :]
    cos_tab = jnp.cos(angles)[:, None, :]
    sin_tab = jnp.sin(angles)[:, None, :]
    vals_f32 = heads_in.astype(jnp.float32)
    first_half = vals_f32[..., :half_dim]
    second_half = vals_f32[..., half_dim:]
    rotated = jnp.concatenate([first_half * cos_tab - second_half * sin_tab, second_half * cos_tab + first_half * sin_tab], axis=-1)
    return rotated.astype(jnp.bfloat16)


def attention_block(x_dev, w_qkv, w_out):
    normed = rms_norm(x_dev).reshape(TOKENS, MODEL_DIM)
    qkv_proj = jnp.dot(normed, w_qkv, preferred_element_type=jnp.float32).astype(jnp.bfloat16)
    qkv_proj = qkv_proj.reshape(BATCH_DEV, SEQ_LEN, 3, NUM_HEADS, HEAD_DIM)
    positions = jnp.arange(SEQ_LEN).astype(jnp.float32)
    query_rot = rotary_embed(qkv_proj[:, :, 0], positions).astype(jnp.float32)
    key_rot = rotary_embed(qkv_proj[:, :, 1], positions).astype(jnp.float32)
    value_heads = qkv_proj[:, :, 2].astype(jnp.float32)
    scores = jnp.einsum("bqhd,bkhd->bhqk", query_rot, key_rot) * (HEAD_DIM ** -0.5)
    causal = jnp.arange(SEQ_LEN)[:, None] >= jnp.arange(SEQ_LEN)[None, :]
    attn_probs = jax.nn.softmax(jnp.where(causal, scores, -1e30), axis=-1).astype(jnp.bfloat16)
    attn_mixed = jnp.einsum("bhqk,bkhd->bqhd", attn_probs.astype(jnp.float32), value_heads).astype(jnp.bfloat16)
    attn_out = jnp.dot(attn_mixed.reshape(TOKENS, NUM_HEADS * HEAD_DIM), w_out, preferred_element_type=jnp.float32)
    return (x_dev.reshape(TOKENS, MODEL_DIM).astype(jnp.float32) + attn_out).astype(jnp.bfloat16)


def expert_rows(operands):
    rows_in, gate_w, up_w, down_w = operands
    gate_act = jnp.dot(rows_in, gate_w, preferred_element_type=jnp.float32)
    up_act = jnp.dot(rows_in, up_w, preferred_element_type=jnp.float32)
    inner_act = (jax.nn.silu(gate_act) * up_act).astype(jnp.bfloat16)
    return jnp.dot(inner_act, down_w, preferred_element_type=jnp.float32).astype(jnp.bfloat16)


def moe_block(hidden, dev_ids, dev_slots, dev_gates, w_gate, w_up, w_down, ws_gate, ws_up, ws_down):
    normed = rms_norm(hidden)
    kept_mask = dev_slots >= 0
    row_index = dev_ids * CAPACITY + dev_slots
    target = jnp.where(kept_mask, row_index, NUM_EXPERTS * CAPACITY).reshape(-1)
    source_tok = jnp.arange(TOKENS * TOP_K, dtype=jnp.int32) // TOP_K
    row_source = jnp.full((NUM_EXPERTS * CAPACITY,), TOKENS, jnp.int32).at[target].set(source_tok, mode="drop")
    buffer = jnp.take(normed, row_source, axis=0, mode="fill", fill_value=0).reshape(NUM_EXPERTS, CAPACITY, MODEL_DIM)
    expert_out = lax.map(expert_rows, (buffer, w_gate, w_up, w_down)).reshape(NUM_EXPERTS * CAPACITY, MODEL_DIM)
    picked = jnp.take(expert_out, jnp.where(kept_mask, row_index, 0), axis=0).astype(jnp.float32)
    weight = jnp.where(kept_mask, dev_gates.astype(jnp.float32), 0.0)
    routed = jnp.sum(weight[:, :, None] * picked, axis=1)
    shared_act = jax.nn.silu(jnp.dot(normed, ws_gate, preferred_element_type=jnp.float32)) * jnp.dot(normed, ws_up, preferred_element_type=jnp.float32)
    shared_out = jnp.dot(shared_act.astype(jnp.bfloat16), ws_down, preferred_element_type=jnp.float32)
    return (hidden.astype(jnp.float32) + shared_out + routed).astype(jnp.bfloat16)


def reference(x_in, w_qkv, w_out, w_gate, w_up, w_down, ws_gate, ws_up, ws_down, expert_ids, slot_ids, gate_vals):
    def per_device(operands):
        x_dev, dev_ids, dev_slots, dev_gates = operands
        hidden = attention_block(x_dev, w_qkv, w_out)
        return moe_block(hidden, dev_ids, dev_slots, dev_gates, w_gate, w_up, w_down, ws_gate, ws_up, ws_down)

    stacked = (x_in.reshape(GROUP_DEVS, BATCH_DEV, SEQ_LEN, MODEL_DIM), expert_ids.reshape(GROUP_DEVS, TOKENS, TOP_K), slot_ids.reshape(GROUP_DEVS, TOKENS, TOP_K), gate_vals.reshape(GROUP_DEVS, TOKENS, TOP_K))
    out_rows = lax.map(per_device, stacked)
    return out_rows.reshape(GROUP_DEVS * BATCH_DEV, SEQ_LEN, MODEL_DIM)
```

```python
import functools

import jax
import jax.numpy as jnp
from jax import lax
from jax.experimental import pallas as pl
from jax.experimental.pallas import tpu as pltpu
from jax.sharding import PartitionSpec as P

HEAD_DIM = 128
ROPE_BASE = 10000.0
EPSILON = 1e-6
VMEM_LIMIT = 60 * 1024 * 1024
F32 = jnp.float32
BF16 = jnp.bfloat16
EXPERT_CHUNKS = (2, 3, 3) + (1,) * 7
BACK_TILES = (1, 3, 3, 1)


def rms_norm(values):
    vals_f32 = values.astype(F32)
    mean_sq = jnp.mean(vals_f32 * vals_f32, axis=-1, keepdims=True)
    return (vals_f32 * lax.rsqrt(mean_sq + EPSILON)).astype(BF16)


def dot32(a, b):
    return jnp.dot(a, b, preferred_element_type=F32)


def cost(flops, nbytes):
    return pl.CostEstimate(flops=flops, bytes_accessed=nbytes, transcendentals=0)


def params(n_axes):
    return pltpu.CompilerParams(dimension_semantics=("arbitrary",) * n_axes, vmem_limit_bytes=VMEM_LIMIT)


def half_cols(ref, side, half):
    return ref[:, pl.ds(pl.multiple_of(side * half, half), half)]


def qkv_kernel(side_ref, a_ref, w_own_ref, w_oth_ref, out_ref):
    side = side_ref[0]
    half = w_own_ref.shape[0]
    acc = dot32(half_cols(a_ref, side, half), w_own_ref[...])
    acc += dot32(half_cols(a_ref, 1 - side, half), w_oth_ref[...])
    out_ref[...] = acc.astype(BF16)


def qkv_matmul(side, a, w_own, w_oth, tile_m=1024, tile_n=768):
    m, k = a.shape
    n = w_own.shape[1]
    spec = pltpu.PrefetchScalarGridSpec(
        num_scalar_prefetch=1,
        grid=(m // tile_m, n // tile_n),
        in_specs=[
            pl.BlockSpec((tile_m, k), lambda i, j, s: (i, 0)),
            pl.BlockSpec((k // 2, tile_n), lambda i, j, s: (0, j)),
            pl.BlockSpec((k // 2, tile_n), lambda i, j, s: (0, j)),
        ],
        out_specs=pl.BlockSpec((tile_m, tile_n), lambda i, j, s: (i, j)),
    )
    price = cost(2 * m * n * k, 2 * (m * k + n * k + m * n))
    return pl.pallas_call(qkv_kernel, grid_spec=spec, out_shape=jax.ShapeDtypeStruct((m, n), BF16), compiler_params=params(2), cost_estimate=price)(side, a, w_own, w_oth)


def attn_kernel(cos_ref, sin_ref, q_ref, k_ref, v_ref, out_ref, *, n_heads):
    cos_tab = cos_ref[...]
    sin_tab = sin_ref[...]
    seq = cos_tab.shape[0]
    block = seq // 2

    def rotate(vals):
        vals = vals.astype(F32)
        return (vals * cos_tab + pltpu.roll(vals, HEAD_DIM // 2, 1) * sin_tab).astype(BF16)

    for head in range(n_heads):
        cols = slice(head * HEAD_DIM, (head + 1) * HEAD_DIM)
        query = rotate(q_ref[:, cols])
        key = rotate(k_ref[:, cols])
        value = v_ref[:, cols]
        for part in range(2):
            n_keys = (part + 1) * block
            scores = lax.dot_general(query[part * block:(part + 1) * block], key[:n_keys], (((1,), (1,)), ((), ())), preferred_element_type=F32)
            scores = scores * (HEAD_DIM ** -0.5)
            q_pos = lax.broadcasted_iota(jnp.int32, scores.shape, 0) + part * block
            k_pos = lax.broadcasted_iota(jnp.int32, scores.shape, 1)
            scores = jnp.where(q_pos >= k_pos, scores, -1e30)
            top = jnp.max(scores, axis=-1, keepdims=True)
            weights = jnp.exp(scores - top)
            total = jnp.sum(weights, axis=-1, keepdims=True)
            probs = (weights * (1.0 / total)).astype(BF16)
            out_ref[part * block:(part + 1) * block, cols] = dot32(probs, value[:n_keys]).astype(BF16)


def attention(qkv, seq_len, heads_step=4):
    m, n = qkv.shape
    n_heads = n // (3 * HEAD_DIM)
    groups = n_heads // heads_step
    half = HEAD_DIM // 2
    inv_freq = ROPE_BASE ** (-jnp.arange(half, dtype=F32) * (2.0 / HEAD_DIM))
    angles = jnp.arange(seq_len, dtype=F32)[:, None] * inv_freq[None, :]
    cos_tab = jnp.concatenate([jnp.cos(angles), jnp.cos(angles)], axis=1)
    sin_tab = jnp.concatenate([-jnp.sin(angles), jnp.sin(angles)], axis=1)
    width = heads_step * HEAD_DIM
    tab_spec = pl.BlockSpec((seq_len, HEAD_DIM), lambda b, g: (0, 0))
    price = cost(4 * m * seq_len * n // 3, 2 * m * n * 4 // 3)
    return pl.pallas_call(
        functools.partial(attn_kernel, n_heads=heads_step),
        grid=(m // seq_len, groups),
        in_specs=[
            tab_spec,
            tab_spec,
            pl.BlockSpec((seq_len, width), lambda b, g: (b, g)),
            pl.BlockSpec((seq_len, width), lambda b, g: (b, groups + g)),
            pl.BlockSpec((seq_len, width), lambda b, g: (b, 2 * groups + g)),
        ],
        out_specs=pl.BlockSpec((seq_len, width), lambda b, g: (b, g)),
        out_shape=jax.ShapeDtypeStruct((m, n // 3), BF16),
        compiler_params=params(2),
        cost_estimate=price,
    )(cos_tab, sin_tab, qkv, qkv, qkv)


def out_kernel(side_ref, o_ref, x_ref, w_own_ref, w_oth_ref, h_ref, u_ref):
    side = side_ref[0]
    half = w_own_ref.shape[0]
    acc = dot32(half_cols(o_ref, side, half), w_own_ref[...])
    acc += dot32(half_cols(o_ref, 1 - side, half), w_oth_ref[...])
    hidden = (x_ref[...].astype(F32) + acc).astype(BF16)
    h_ref[...] = hidden
    u_ref[...] = rms_norm(hidden)


def out_project(side, mixed, x, w_own, w_oth, tile_m=512):
    m, k = mixed.shape
    n = w_own.shape[1]
    row_spec = pl.BlockSpec((tile_m, n), lambda i, s: (i, 0))
    spec = pltpu.PrefetchScalarGridSpec(
        num_scalar_prefetch=1,
        grid=(m // tile_m,),
        in_specs=[
            pl.BlockSpec((tile_m, k), lambda i, s: (i, 0)),
            row_spec,
            pl.BlockSpec((k // 2, n), lambda i, s: (0, 0)),
            pl.BlockSpec((k // 2, n), lambda i, s: (0, 0)),
        ],
        out_specs=[row_spec, row_spec],
    )
    price = cost(2 * m * n * k, 2 * (4 * m * k + n * k))
    shape = jax.ShapeDtypeStruct((m, n), BF16)
    return pl.pallas_call(out_kernel, grid_spec=spec, out_shape=[shape, shape], compiler_params=params(1), cost_estimate=price)(side, mixed, x, w_own, w_oth)


def shared_kernel(side_ref, u_ref, g_own_ref, g_oth_ref, p_own_ref, p_oth_ref, down_ref, z_ref):
    side = side_ref[0]
    half = g_own_ref.shape[0]
    u_own = half_cols(u_ref, side, half)
    u_oth = half_cols(u_ref, 1 - side, half)
    gate = dot32(u_own, g_own_ref[...]) + dot32(u_oth, g_oth_ref[...])
    up = dot32(u_own, p_own_ref[...]) + dot32(u_oth, p_oth_ref[...])
    inner = (jax.nn.silu(gate) * up).astype(BF16)
    part = dot32(inner, down_ref[...])

    @pl.when(pl.program_id(1) == 0)
    def _():
        z_ref[...] = part

    @pl.when(pl.program_id(1) > 0)
    def _():
        z_ref[...] += part


def shared_ffn(side, u, g_own, g_oth, p_own, p_oth, down, tile_m=1024, tile_f=512):
    m, k = u.shape
    ff = g_own.shape[1]
    n = down.shape[1]
    w_spec = pl.BlockSpec((k // 2, tile_f), lambda i, f, s: (0, f))
    spec = pltpu.PrefetchScalarGridSpec(
        num_scalar_prefetch=1,
        grid=(m // tile_m, ff // tile_f),
        in_specs=[pl.BlockSpec((tile_m, k), lambda i, f, s: (i, 0)), w_spec, w_spec, w_spec, w_spec, pl.BlockSpec((tile_f, n), lambda i, f, s: (f, 0))],
        out_specs=pl.BlockSpec((tile_m, n), lambda i, f, s: (i, 0)),
    )
    price = cost(2 * m * ff * (2 * k + n), 2 * (m * k + 2 * ff * k + ff * n) + 4 * m * n)
    return pl.pallas_call(shared_kernel, grid_spec=spec, out_shape=jax.ShapeDtypeStruct((m, n), F32), compiler_params=params(2), cost_estimate=price)(side, u, g_own, g_oth, p_own, p_oth, down)


def expert_kernel(place_ref, count_ref, rows_ref, g_own_ref, g_oth_ref, p_own_ref, p_oth_ref, down_ref, *y_refs, source, sizes, first):
    side = place_ref[0]
    half = g_own_ref.shape[1]
    step = pl.program_id(1)
    token_side, src = source(step, place_ref)
    count = count_ref[first + pl.program_id(0), token_side * (count_ref.shape[1] // 2) + src]
    col_own = pl.ds(pl.multiple_of(side * half, half), half)
    col_oth = pl.ds(pl.multiple_of((1 - side) * half, half), half)
    lead = (0,) * (len(y_refs[0].shape) - 2)
    cap = y_refs[0].shape[-2]

    def run(size):
        r_own = rows_ref[0, 0, 0, :size, col_own]
        r_oth = rows_ref[0, 0, 0, :size, col_oth]
        gate = dot32(r_own, g_own_ref[0]) + dot32(r_oth, g_oth_ref[0])
        up = dot32(r_own, p_own_ref[0]) + dot32(r_oth, p_oth_ref[0])
        inner = (jax.nn.silu(gate) * up).astype(BF16)
        y = dot32(inner, down_ref[0])
        filled = lax.broadcasted_iota(jnp.int32, y.shape, 0) < count
        y = jnp.where(filled, y, 0.0).astype(BF16)
        for i, y_ref in enumerate(y_refs):
            @pl.when((step == i) | (len(y_refs) == 1))
            def _(y_ref=y_ref):
                y_ref[lead + (slice(0, size),)] = y
                if size < cap:
                    y_ref[lead + (slice(size, cap),)] = jnp.zeros((cap - size, y.shape[1]), BF16)

    for low, size in zip((-1,) + sizes[:-1], sizes):
        @pl.when((count > low) & (count <= size))
        def _():
            run(size)


def expert_ffn(place, counts, rows, w_gate, w_up, gate_oth, up_oth, w_down, first, only=None):
    _, n_src, _, cap, k = rows.shape
    n_exp, _, ff = gate_oth.shape
    n = w_down.shape[2]

    if only is None:
        steps = 2 * n_src
        source = lambda d, place: (d // n_src, lax.rem(d, n_src))
        out_specs = pl.BlockSpec((1, 1, 1, cap, n), lambda e, d, *_: (lax.rem(d, n_src), d // n_src, e, 0, 0))
        out_shape = jax.ShapeDtypeStruct((n_src, 2, n_exp, cap, n), BF16)
    else:
        token_side, shift, steps = only
        source = lambda d, place: (token_side, place[1] ^ (d + shift))
        out_specs = [pl.BlockSpec((cap, n), lambda *_: (0, 0))] * steps
        out_shape = [jax.ShapeDtypeStruct((cap, n), BF16)] * steps
    w_spec = pl.BlockSpec((1, k // 2, ff), lambda e, *_: (first + e, 0, 0))
    oth_spec = pl.BlockSpec((1, k // 2, ff), lambda e, *_: (e, 0, 0))
    spec = pltpu.PrefetchScalarGridSpec(
        num_scalar_prefetch=2,
        grid=(n_exp, steps),
        in_specs=[
            pl.BlockSpec((1, 1, 1, cap, k), lambda e, d, place, c: source(d, place) + (first + e, 0, 0)),
            w_spec,
            oth_spec,
            w_spec,
            oth_spec,
            pl.BlockSpec((1, ff, n), lambda e, *_: (first + e, 0, 0)),
        ],
        out_specs=out_specs,
    )
    m = steps * n_exp * cap
    price = cost(2 * m * ff * (2 * k + n), 2 * (m * (k + n) + n_exp * ff * (2 * k + n)))
    kern = functools.partial(expert_kernel, source=source, sizes=(128, 192, 256, cap), first=first)
    return pl.pallas_call(kern, grid_spec=spec, out_shape=out_shape, compiler_params=params(2), cost_estimate=price)(
        place, counts, rows, w_gate, gate_oth, w_up, up_oth, w_down
    )


WIN = 64
GROUP = 8
SLOTS = 8
LANES = 128


def windows_kernel(low_ref, high_ref, spot_ref, base_ref, skip_ref, bound_ref, *, chunks, n_src, cap, room):
    n_exp = low_ref.shape[1]
    per_src = n_exp // n_src
    n_bound = len(chunks) + 1

    def tile_step(tile, _):
        at, first = tile * room, 0
        for part, size in enumerate(chunks):
            bound_ref[tile * n_bound + part] = at - tile * room

            def expert_step(i, at, size=size, first=first):
                src = i // size
                local = i - src * size
                e = src * per_src + first + local
                high = high_ref[tile, e]

                def push(state):
                    pos, at = state
                    start = jnp.minimum(pos // 16 * 16, cap - WIN)
                    spot_ref[at] = (src * 64 + local) * 1024 + start
                    base_ref[at] = e * cap + start
                    skip_ref[at] = pos - start
                    return start + WIN, at + 1

                return lax.while_loop(lambda st: st[0] < high, push, (low_ref[tile, e], at))[1]

            at = lax.fori_loop(0, n_src * size, expert_step, at)
            first += size
        n_win = at - tile * room
        bound_ref[tile * n_bound + n_bound - 1] = n_win

        def pad(i, _):
            spot_ref[at + i] = 0
            base_ref[at + i] = 0
            skip_ref[at + i] = WIN
            return 0

        return lax.fori_loop(0, (n_win + 4 * GROUP - 1) // (2 * GROUP) * (2 * GROUP) - n_win, pad, 0)

    lax.fori_loop(0, low_ref.shape[0], tile_step, 0)


def list_room(n_exp, tile_rows):
    return 2 * n_exp + tile_rows // WIN + 4 * GROUP


def list_windows(low, high, chunks, n_src, cap, tile_rows):
    n_tiles, n_exp = low.shape
    room = list_room(n_exp, tile_rows)
    smem = pl.BlockSpec(memory_space=pltpu.SMEM)
    shapes = [jax.ShapeDtypeStruct((n_tiles * room,), jnp.int32)] * 3 + [jax.ShapeDtypeStruct((n_tiles * (len(chunks) + 1),), jnp.int32)]
    kern = functools.partial(windows_kernel, chunks=chunks, n_src=n_src, cap=cap, room=room)
    price = cost(n_tiles * 2000000000, n_tiles * room * 12)
    return pl.pallas_call(kern, in_specs=[smem, smem], out_specs=[smem] * 4, out_shape=shapes, cost_estimate=price)(low, high)


def combine_kernel(place_ref, spot_ref, base_ref, skip_ref, bound_ref, rows_ref, gates_ref, h_ref, z_ref, *rest, who, list_tile, n_part, room):
    y_refs, last_refs = rest[:n_part - 1], rest[n_part - 1:-8]
    out_ref, acc, buf, pick_a, pick_b, row_wide, gate_wide, sems = rest[-8:]
    step = pl.program_id(0)
    limit = SLOTS * GROUP

    def start_one(part, tile, at, parity):
        spot = spot_ref[tile * room + at]
        group = parity * SLOTS + lax.rem(at // GROUP, SLOTS)
        src = spot // 65536
        rows = pl.ds(pl.multiple_of(spot % 1024, 16), WIN)

        def go(ref):
            pltpu.make_async_copy(ref, buf.at[group, pl.ds(pl.multiple_of(lax.rem(at, GROUP) * WIN, WIN), WIN), :], sems.at[group]).start()

        if part < n_part - 1:
            go(y_refs[part].at[src, who, spot // 1024 % 64, rows, :])
        else:
            for i, ref in enumerate(last_refs):
                @pl.when((src ^ place_ref[1]) == i)
                def _(ref=ref):
                    go(ref.at[rows, :])

    def start_range(tile, parity, low, high):
        def loop(part, first, last):
            def one(at, _):
                start_one(part, tile, at, parity)
                return 0

            lax.fori_loop(jnp.maximum(first, low), jnp.minimum(last, high), one, 0)

        bounds = [bound_ref[tile * (n_part + 1) + p] for p in range(n_part + 1)]
        for part in range(n_part):
            loop(part, bounds[part], bounds[part + 1])
        loop(0, bounds[n_part], pairs_of(tile) * 2 * GROUP)

    def pairs_of(tile):
        return (bound_ref[tile * (n_part + 1) + n_part] + 2 * GROUP - 1) // (2 * GROUP)

    tile = list_tile + step
    parity = lax.rem(step, 2)

    @pl.when(step == 0)
    def _():
        start_range(tile, 0, 0, limit)

    @pl.when(step + 1 < pl.num_programs(0))
    def _():
        start_range(tile + 1, 1 - parity, 0, limit)

    lane = lax.broadcasted_iota(jnp.int32, (1, LANES), 1)
    per_lane = LANES // WIN

    def build(group, pick):
        for part in range(GROUP // per_lane):
            ids = jnp.full((1, LANES), -2, jnp.int32)
            for w in range(per_lane):
                at = tile * room + group * GROUP + part * per_lane + w
                inside = (lane >= w * WIN + skip_ref[at]) & (lane < (w + 1) * WIN)
                ids = jnp.where(inside, base_ref[at] - w * WIN + lane, ids)
            value = jnp.zeros(row_wide.shape[1:], F32)
            for k in range(row_wide.shape[0]):
                value = jnp.where(row_wide[k] == ids, gate_wide[k], value)
            pick[:, part * LANES:(part + 1) * LANES] = value.astype(BF16)

    def wait(group):
        slot = parity * SLOTS + lax.rem(group, SLOTS)
        pltpu.make_async_copy(buf.at[slot], buf.at[slot], sems.at[slot]).wait()
        return buf.at[slot]

    acc[...] = h_ref[...].astype(F32) + z_ref[...]
    for k in range(row_wide.shape[0]):
        row_wide[k] = jnp.broadcast_to(rows_ref[:, k:k + 1], row_wide.shape[1:])
        gate_wide[k] = jnp.broadcast_to(gates_ref[:, k:k + 1], gate_wide.shape[1:])
    n_pairs = pairs_of(tile)
    build(0, pick_a)

    def pair_step(p, _):
        buf_a, buf_b = wait(2 * p), wait(2 * p + 1)
        build(2 * p + 1, pick_b)
        acc[...] += dot32(pick_a[...], buf_a[...])
        build(2 * p + 2, pick_a)
        acc[...] += dot32(pick_b[...], buf_b[...])
        ahead = (2 * p + SLOTS) * GROUP

        @pl.when(ahead < n_pairs * 2 * GROUP)
        def _():
            start_range(tile, parity, ahead, ahead + 2 * GROUP)

        return 0

    lax.fori_loop(0, n_pairs, pair_step, 0)
    out_ref[...] = acc[...].astype(BF16)


def combine(place, lists, list_tile, rows, gates, hidden, z, parts, last_parts, who, first_tile, n_tiles, tile_m, whole=False):
    m, _ = hidden.shape
    n = z.shape[1]
    top_k = rows.shape[1]
    n_exp = parts[0].shape[0] * sum(EXPERT_CHUNKS)
    room = list_room(n_exp, tile_m * top_k)
    at = lambda i, *_: (first_tile + i, 0)
    spec = pltpu.PrefetchScalarGridSpec(
        num_scalar_prefetch=5,
        grid=(n_tiles,),
        in_specs=[
            pl.BlockSpec((tile_m, top_k), at),
            pl.BlockSpec((tile_m, top_k), at),
            pl.BlockSpec((tile_m, n), lambda i, s, *_: (first_tile + i, s[0])),
            pl.BlockSpec((tile_m, n), at),
        ]
        + [pl.BlockSpec(memory_space=pl.ANY)] * (len(parts) + len(last_parts)),
        out_specs=pl.BlockSpec((tile_m, n), lambda i, s, *_: (first_tile + i if whole else i, s[0] if whole else 0)),
        scratch_shapes=[
            pltpu.VMEM((tile_m, n), F32),
            pltpu.VMEM((2 * SLOTS, GROUP * WIN, n), BF16),
            pltpu.VMEM((tile_m, GROUP * WIN), BF16),
            pltpu.VMEM((tile_m, GROUP * WIN), BF16),
            pltpu.VMEM((top_k, tile_m, LANES), jnp.int32),
            pltpu.VMEM((top_k, tile_m, LANES), F32),
            pltpu.SemaphoreType.DMA((2 * SLOTS,)),
        ],
    )
    work = n_tiles * WIN * n_exp
    price = cost(2 * work * tile_m * n, 2 * work * n + 8 * n_tiles * tile_m * n)
    kern = functools.partial(combine_kernel, who=who, list_tile=list_tile, n_part=len(parts) + 1, room=room)
    shape = (m, 2 * n) if whole else (n_tiles * tile_m, n)
    return pl.pallas_call(kern, grid_spec=spec, out_shape=jax.ShapeDtypeStruct(shape, BF16), compiler_params=params(1), cost_estimate=price)(
        place, *lists, rows, gates, hidden, z, *parts, *last_parts
    )


def place_kernel(side_ref, piece_ref, out_in_ref, out_ref):
    out_ref[...] = piece_ref[...]


def place(side, piece, out, first_tile, tile_m):
    n_tiles, n = piece.shape[0] // tile_m, piece.shape[1]
    spec = pltpu.PrefetchScalarGridSpec(
        num_scalar_prefetch=1,
        grid=(n_tiles,),
        in_specs=[pl.BlockSpec((tile_m, n), lambda i, s: (i, 0)), pl.BlockSpec(memory_space=pl.ANY)],
        out_specs=pl.BlockSpec((tile_m, n), lambda i, s: (first_tile + i, 1 - s[0])),
    )
    price = cost(n_tiles * tile_m * n, 4 * n_tiles * tile_m * n)
    return pl.pallas_call(place_kernel, grid_spec=spec, out_shape=jax.ShapeDtypeStruct(out.shape, BF16), input_output_aliases={2: 0}, compiler_params=params(1), cost_estimate=price)(
        side, piece, out
    )


DWIN = 32
DGROUP = 16


def dispatch_kernel(base_ref, low_ref, high_ref, rows_ref, u_ref, *rest):
    out_ref, pick, found, win_exp, win_start, win_skip = rest[-6:]
    n_exp, cap = out_ref.shape[2], out_ref.shape[3]
    step = pl.program_id(0) * pl.num_programs(1) + pl.program_id(1)
    tile = u_ref.shape[0]

    def list_expert(e, n_win):
        high = high_ref[step, e]

        def push(state):
            pos, n_win = state
            start = jnp.minimum(pos // 16 * 16, cap - DWIN)
            win_exp[n_win] = e
            win_start[n_win] = start
            win_skip[n_win] = pos - start
            return start + DWIN, n_win + 1

        return lax.while_loop(lambda st: st[0] < high, push, (low_ref[step, e], n_win))[1]

    n_win = lax.fori_loop(0, n_exp, list_expert, jnp.int32(0))
    row = lax.broadcasted_iota(jnp.int32, (DWIN, tile), 0)
    picks = [rows_ref[0, k:k + 1, :] for k in range(rows_ref.shape[1])]

    def group_step(group, _):
        for w in range(DGROUP):
            at = group * DGROUP + w

            @pl.when(at < n_win)
            def _():
                ids = row + ((base_ref[0] + win_exp[at]) * cap + win_start[at])
                hit = picks[0] == ids
                for other in picks[1:]:
                    hit |= other == ids
                pick[w * DWIN:(w + 1) * DWIN, :] = jnp.where(hit, 1.0, 0.0).astype(BF16)

        found[...] = dot32(pick[...], u_ref[...]).astype(BF16)
        for w in range(DGROUP):
            at = group * DGROUP + w

            @pl.when(at < n_win)
            def _():
                spot = pl.ds(pl.multiple_of(win_start[at], 16), DWIN)
                e = win_exp[at]
                old = out_ref[0, 0, e, spot, :]
                fresh = lax.broadcasted_iota(jnp.int32, old.shape, 0) >= win_skip[at]
                out_ref[0, 0, e, spot, :] = jnp.where(fresh, found[w * DWIN:(w + 1) * DWIN, :], old)

        return 0

    lax.fori_loop(0, (n_win + DGROUP - 1) // DGROUP, group_step, 0)


def dispatch(base, low, high, rows, u, cap, which, filled=None):
    n_src, n_tiles, n_exp = low.shape
    top_k = rows.shape[1]
    m, k = u.shape
    tile = m // (n_src * n_tiles)
    max_win = 2 * n_exp + tile * top_k // DWIN + DGROUP
    more = () if filled is None else (filled,)
    spec = pltpu.PrefetchScalarGridSpec(
        num_scalar_prefetch=3,
        grid=(n_src, n_tiles),
        in_specs=[
            pl.BlockSpec((1, top_k, tile), lambda d, t, *s: (d, 0, t)),
            pl.BlockSpec((tile, k), lambda d, t, *s: (d * n_tiles + t, 0)),
        ]
        + [pl.BlockSpec(memory_space=pl.ANY)] * len(more),
        out_specs=pl.BlockSpec((1, 1, n_exp, cap, k), lambda d, t, *s: (which, d, 0, 0, 0)),
        scratch_shapes=[pltpu.VMEM((DGROUP * DWIN, tile), BF16), pltpu.VMEM((DGROUP * DWIN, k), BF16)] + [pltpu.SMEM((max_win,), jnp.int32)] * 3,
    )
    price = cost(2 * n_src * n_tiles * DGROUP * DWIN * tile * k, 2 * m * k + 2 * n_src * n_exp * cap * k)
    return pl.pallas_call(dispatch_kernel, grid_spec=spec, out_shape=jax.ShapeDtypeStruct((2, n_src, n_exp, cap, k), BF16), input_output_aliases={5: 0} if more else {}, compiler_params=params(2), cost_estimate=price)(
        base, low.reshape(-1, n_exp), high.reshape(-1, n_exp), rows, u, *more
    )


def capacity_for(n_tokens, top_k, n_experts):
    return ((5 * n_tokens * top_k) // (4 * n_experts) + 7) // 8 * 8


def solution(mesh):
    n_ep = mesh.shape["ep"]
    n_side = mesh.shape["fsdp"]
    tok_spec = P(("data", "fsdp", "ep"))
    row_spec = P("fsdp", None)
    swap = [(0, 1), (1, 0)]
    tile_m, small_m = 512, 256

    def local_step(x_in, w_qkv, w_out, w_gate, w_up, w_down, ws_gate, ws_up, ws_down, expert_ids, slot_ids, gate_vals):
        side = lax.axis_index("fsdp")
        ep = lax.axis_index("ep")
        place_arr = jnp.stack([side, ep]).astype(jnp.int32)
        n_batch, seq_len, model_dim = x_in.shape
        n_tokens = n_batch * seq_len
        top_k = expert_ids.shape[-1]
        n_local = w_gate.shape[0]
        n_experts = n_local * n_ep
        n_tiles = n_tokens // tile_m
        n_small = n_tokens // small_m
        cap = (capacity_for(n_tokens, top_k, n_experts) + 15) // 16 * 16

        def quarter(w):
            q = w.shape[0] // n_ep
            return lax.ppermute(lax.dynamic_slice_in_dim(w, ep * q, q, 0), "fsdp", swap)

        def spread(w):
            return lax.all_gather(w, "ep", axis=0, tiled=True)

        qkv_q = quarter(w_qkv)
        out_q = quarter(w_out)
        sg_q = quarter(ws_gate)
        su_q = quarter(ws_up)

        def send_weights(chunk, gate_w, up_w):
            first = sum(EXPERT_CHUNKS[:chunk])
            last = first + EXPERT_CHUNKS[chunk]
            gate_oth = lax.ppermute(gate_w[first:last], "fsdp", swap)
            return first, gate_oth, lax.ppermute(up_w[first:last], "fsdp", swap)

        sent = [send_weights(0, w_gate, w_up)]
        ids = expert_ids.reshape(n_tokens, top_k)
        slots = slot_ids.reshape(n_tokens, top_k)
        kept = slots >= 0
        rows = jnp.where(kept, ids * cap + slots, -1)
        gates = jnp.where(kept, gate_vals.reshape(n_tokens, top_k).astype(F32), 0.0)
        hits = (ids.reshape(n_small, -1, 1) == jnp.arange(n_experts, dtype=jnp.int32)) & kept.reshape(n_small, -1, 1)
        high = jnp.cumsum(jnp.sum(hits.astype(jnp.int32), axis=1), axis=0)
        table = jnp.concatenate([rows.T.reshape(-1), high.reshape(-1)])
        table_p = lax.ppermute(table, "fsdp", swap)
        gates_p = lax.ppermute(gates, "fsdp", swap)
        tables = lax.all_gather(jnp.stack([table, table_p]), "ep", axis=0)

        def split(tab):
            lead = tab.shape[:-1]
            r = tab[..., :n_tokens * top_k].reshape(lead + (top_k, n_tokens))
            hi = tab[..., n_tokens * top_k:].reshape(lead + (n_small, n_experts))
            lo = jnp.concatenate([jnp.zeros_like(hi[..., :1, :]), hi[..., :-1, :]], axis=-2)
            return r, lo, hi

        rows_all, low_all, high_all = split(tables)
        low_all, high_all = [lax.dynamic_slice_in_dim(v, ep * n_local, n_local, 3) for v in (low_all, high_all)]
        counts = jnp.transpose(high_all[:, :, -1, :], (2, 1, 0)).reshape(n_local, n_side * n_ep)
        rows_p, low_p, high_p = split(table_p)
        rows_p = rows_p.T
        _, low, high = split(table)
        per = n_small // n_tiles
        low, high, low_p, high_p = low[::per], high[per - 1::per], low_p[::per], high_p[per - 1::per]
        base = jnp.full((1,), ep * n_local, jnp.int32)

        x_flat = x_in.reshape(n_tokens, model_dim)
        normed = rms_norm(x_flat)
        qkv_oth = spread(qkv_q)
        qkv = qkv_matmul(place_arr, normed, w_qkv, qkv_oth)
        mixed = attention(qkv, seq_len)
        out_oth = spread(out_q)
        hidden, u_own = out_project(place_arr, mixed, x_flat, w_out, out_oth)
        hidden_p = lax.ppermute(hidden, "fsdp", swap)
        all_own = spread(u_own)
        u_par = rms_norm(hidden_p)
        all_par = spread(u_par)
        sg_oth = spread(sg_q)
        su_oth = spread(su_q)
        z_own = shared_ffn(place_arr, u_own, ws_gate, sg_oth, ws_up, su_oth, ws_down)
        late_gate, late_up, z_own = lax.optimization_barrier((w_gate, w_up, z_own))
        sent += [send_weights(i, late_gate, late_up) for i in range(1, len(EXPERT_CHUNKS))]
        z_par = shared_ffn(place_arr, u_par, ws_gate, sg_oth, ws_up, su_oth, ws_down)
        rows_buf = dispatch(base, low_all[:, 0], high_all[:, 0], rows_all[:, 0], all_own, cap, 0)
        rows_buf = dispatch(base, low_all[:, 1], high_all[:, 1], rows_all[:, 1], all_par, cap, 1, rows_buf)

        parts = []
        for first, gate_oth, up_oth in sent[:-1]:
            y = expert_ffn(place_arr, counts, rows_buf, w_gate, w_up, gate_oth, up_oth, w_down, first)
            parts.append(lax.all_to_all(y, "ep", 0, 0, tiled=True))
        first, gate_oth, up_oth = sent[-1]
        last_parts = [[None] * n_ep, [None] * n_ep]
        half_ep = n_ep // 2
        for who, shift in ((1, half_ep), (1, 0), (0, half_ep), (0, 0)):
            rows_out = expert_ffn(place_arr, counts, rows_buf, w_gate, w_up, gate_oth, up_oth, w_down, first, (who, shift, half_ep))
            for i, y in enumerate(rows_out):
                step = shift + i
                last_parts[who][step] = lax.ppermute(y, "ep", [(j, j ^ step) for j in range(n_ep)]) if step else y

        lists = list_windows(jnp.concatenate([low, low_p]), jnp.concatenate([high, high_p]), EXPERT_CHUNKS, n_ep, cap, tile_m * top_k)
        back, tile = [], n_tiles
        for size in BACK_TILES:
            tile -= size
            piece = combine(place_arr, lists, n_tiles + tile, rows_p, gates_p, hidden_p, z_par, parts, last_parts[1], 1, tile, size, tile_m)
            back.append((lax.ppermute(piece, "fsdp", swap), tile))
        out = combine(place_arr, lists, 0, rows, gates, hidden, z_own, parts, last_parts[0], 0, 0, n_tiles, tile_m, whole=True)
        for piece, tile in back:
            out = place(place_arr, piece, out, tile, tile_m)
        return out.reshape(n_batch, seq_len, model_dim)

    return jax.shard_map(local_step, mesh=mesh, in_specs=(tok_spec, row_spec, row_spec, P("ep", "fsdp", None), P("ep", "fsdp", None), P("ep", None, "fsdp"), row_spec, row_spec, P(None, "fsdp"), tok_spec, tok_spec, tok_spec), out_specs=tok_spec, check_vma=False)
```
